16 devices in a mesh: data: 2 (over z), stage: 8 (over y, x, core).
Axes of the slice: x: 2, y: 2, z: 2, core: 2. Of those that a mesh axis runs over, the one named last changes fastest.
Arguments:
- x_enc: bfloat16 [16, 1536, 1536], P(('data', 'stage'))
- h_dec: bfloat16 [16, 64, 1536], P(('data', 'stage'))
- cot_out: bfloat16 [16, 64, 1536], P(('data', 'stage'))
- enc_up: bfloat16 [1, 1536, 8960], replicated
- enc_down: bfloat16 [1, 8960, 1536], replicated
- w_key: bfloat16 [1, 1536, 2, 128], replicated
- w_val: bfloat16 [1, 1536, 2, 128], replicated
- w_query: bfloat16 [1, 1536, 1536], replicated
- w_out: bfloat16 [1, 1536, 1536], replicated
- w_ff1: bfloat16 [1, 1536, 8960], replicated
- w_ff2: bfloat16 [1, 8960, 1536], replicated
Outputs:
- output 1: bfloat16 [16, 1536, 1536], P(('data', 'stage'))
- output 2: bfloat16 [16, 64, 1536], P(('data', 'stage'))
- output 3: float32 [1, 1536, 8960], P(None, ('data', 'stage'))
- output 4: float32 [1, 8960, 1536], P(None, ('data', 'stage'))
- output 5: float32 [1, 1536, 2, 128], P(None, ('data', 'stage'))
- output 6: float32 [1, 1536, 2, 128], P(None, ('data', 'stage'))
- output 7: float32 [1, 1536, 1536], P(None, ('data', 'stage'))
- output 8: float32 [1, 1536, 1536], P(None, ('data', 'stage'))
- output 9: float32 [1, 1536, 8960], P(None, ('data', 'stage'))
- output 10: float32 [1, 8960, 1536], P(None, ('data', 'stage'))
All inputs are finite; a program needn't handle non-finite values.
Results may differ from the reference program's by a relative error of at most 0.02.
Values are sent between devices in bfloat16 or wider.
A program may use at most 1 GiB of HBM per device.

```python
import jax
import jax.numpy as jnp
from jax import lax

DATA = 2
STAGE = 8
BATCH = 1
S_ENC = 1536
S_DEC = 64
D_MODEL = 1536
HEADS = 12
KV_HEADS = 2
HEAD = 128
FF = 8960
L_ENC = 1
L_DEC = 1
ROWS = DATA * STAGE * BATCH
GROUP = HEADS // KV_HEADS


def draw_normal(key, shape, factor):
    return (jax.random.normal(key, shape, jnp.float32) * factor).astype(jnp.bfloat16)


def setup_inputs(seed: int = 0) -> dict:
    key_list = jax.random.split(jax.random.key(seed), 11)
    return {
        'x_enc': draw_normal(key_list[0], (ROWS, S_ENC, D_MODEL), 1.0),
        'h_dec': draw_normal(key_list[1], (ROWS, S_DEC, D_MODEL), 1.0),
        'cot_out': draw_normal(key_list[2], (ROWS, S_DEC, D_MODEL), 1.0),
        'enc_up': draw_normal(key_list[3], (L_ENC, D_MODEL, FF), D_MODEL ** -0.5),
        'enc_down': draw_normal(key_list[4], (L_ENC, FF, D_MODEL), 1.5 * (FF * L_ENC) ** -0.5),
        'w_key': draw_normal(key_list[5], (L_DEC, D_MODEL, KV_HEADS, HEAD), D_MODEL ** -0.5),
        'w_val': draw_normal(key_list[6], (L_DEC, D_MODEL, KV_HEADS, HEAD), D_MODEL ** -0.5),
        'w_query': draw_normal(key_list[7], (L_DEC, D_MODEL, D_MODEL), D_MODEL ** -0.5),
        'w_out': draw_normal(key_list[8], (L_DEC, D_MODEL, D_MODEL), (S_ENC / (6.0 * D_MODEL * L_DEC)) ** 0.5),
        'w_ff1': draw_normal(key_list[9], (L_DEC, D_MODEL, FF), D_MODEL ** -0.5),
        'w_ff2': draw_normal(key_list[10], (L_DEC, FF, D_MODEL), 1.5 * (FF * L_DEC) ** -0.5),
    }


def mlp_block(hidden, w_a, w_b):
    flat_in = hidden.reshape(-1, D_MODEL)
    pre_act = jnp.dot(flat_in, w_a, preferred_element_type=jnp.float32)
    hidden_act = jax.nn.gelu(pre_act).astype(jnp.bfloat16)
    out_sum = flat_in.astype(jnp.float32) + jnp.dot(hidden_act, w_b, preferred_element_type=jnp.float32)
    return out_sum.astype(jnp.bfloat16).reshape(hidden.shape)


def cross_attention(hidden, k_mem, v_mem, w_q, w_o):
    flat_in = hidden.reshape(-1, D_MODEL)
    query = jnp.dot(flat_in, w_q, preferred_element_type=jnp.float32).astype(jnp.bfloat16)
    query = query.reshape(hidden.shape[0], S_DEC, KV_HEADS, GROUP, HEAD)

    def one_row(operands):
        q_row, k_row, v_row = operands
        logits = jnp.einsum('qkgh,skh->kgqs', q_row.astype(jnp.float32), k_row.astype(jnp.float32)) * HEAD ** -0.5
        attn_prob = jax.nn.softmax(logits, axis=-1).astype(jnp.bfloat16).astype(jnp.float32)
        return jnp.einsum('kgqs,skh->qkgh', attn_prob, v_row.astype(jnp.float32)).astype(jnp.bfloat16)

    context = lax.map(one_row, (query, k_mem, v_mem))
    out_sum = flat_in.astype(jnp.float32) + jnp.dot(context.reshape(-1, D_MODEL), w_o, preferred_element_type=jnp.float32)
    return out_sum.astype(jnp.bfloat16).reshape(hidden.shape)


def forward(x_enc, h_dec, enc_up, enc_down, w_key, w_val, w_query, w_out, w_ff1, w_ff2):
    def enc_step(memory, weights):
        return mlp_block(memory, weights[0], weights[1]), None

    memory = lax.scan(enc_step, x_enc, (enc_up, enc_down))[0]
    paired = jnp.roll(memory.reshape(DATA, STAGE, BATCH, S_ENC, D_MODEL), STAGE // 2, axis=1)
    flat_mem = paired.reshape(ROWS * S_ENC, D_MODEL).astype(jnp.float32)
    key_all = jnp.einsum('nd,ldkh->lnkh', flat_mem, w_key.astype(jnp.float32)).astype(jnp.bfloat16)
    val_all = jnp.einsum('nd,ldkh->lnkh', flat_mem, w_val.astype(jnp.float32)).astype(jnp.bfloat16)
    key_all = key_all.reshape(L_DEC, ROWS, S_ENC, KV_HEADS, HEAD)
    val_all = val_all.reshape(L_DEC, ROWS, S_ENC, KV_HEADS, HEAD)

    def dec_step(hidden, weights):
        k_mem, v_mem, w_q, w_o, w_a, w_b = weights
        mid_out = cross_attention(hidden, k_mem, v_mem, w_q, w_o)
        return mlp_block(mid_out, w_a, w_b), None

    return lax.scan(dec_step, h_dec, (key_all, val_all, w_query, w_out, w_ff1, w_ff2))[0]


def reference(x_enc, h_dec, cot_out, enc_up, enc_down, w_key, w_val, w_query, w_out, w_ff1, w_ff2):
    pull = jax.vjp(forward, x_enc, h_dec, enc_up, enc_down, w_key, w_val, w_query, w_out, w_ff1, w_ff2)[1]
    grad_list = pull(cot_out)
    return (grad_list[0], grad_list[1], grad_list[2].astype(jnp.float32), grad_list[3].astype(jnp.float32),
            grad_list[4].astype(jnp.float32), grad_list[5].astype(jnp.float32), grad_list[6].astype(jnp.float32),
            grad_list[7].astype(jnp.float32), grad_list[8].astype(jnp.float32), grad_list[9].astype(jnp.float32))
```

```python
import jax
import jax.numpy as jnp
from jax import lax
from jax.experimental.layout import Layout, with_layout_constraint
from jax.sharding import PartitionSpec as P


F32 = jnp.float32
BF16 = jnp.bfloat16
AXES = ('data', 'stage')


def dot(lhs, rhs, lhs_dim, rhs_dim):
    return lax.dot_general(lhs, rhs, (((lhs_dim,), (rhs_dim,)), ((), ())), preferred_element_type=F32)


def bdot(lhs, rhs, lhs_dim, rhs_dim):
    return lax.dot_general(lhs, rhs, (((lhs_dim,), (rhs_dim,)), ((0,), (0,))), preferred_element_type=F32)


def gather(rows):
    return lax.all_gather(rows, AXES, axis=0, tiled=True)


def scatter(own):
    return lax.psum_scatter(own, AXES, scatter_dimension=0, tiled=True)


def solution(mesh):
    stage_size = mesh.shape['stage']
    n_dev = mesh.shape['data'] * stage_size
    partner_perm = [(index, (index + stage_size // 2) % stage_size) for index in range(stage_size)]
    row_spec = P(AXES, None, None)
    full_spec3 = P(None, None, None)
    full_spec4 = P(None, None, None, None)
    grad_spec3 = P(None, AXES, None)
    grad_spec4 = P(None, AXES, None, None)

    def step(x_enc, h_dec, cot_out, enc_up, enc_down, w_key, w_val, w_query, w_out, w_ff1, w_ff2):
        d_model = x_enc.shape[-1]
        kv_heads, head = w_key.shape[2], w_key.shape[3]
        group = d_model // (kv_heads * head)
        kv_width = kv_heads * head
        x, up, down = x_enc[0], enc_up[0], enc_down[0]
        w_q, w_o, w_1, w_2 = w_query[0], w_out[0], w_ff1[0], w_ff2[0]
        w_kv = jnp.concatenate([w_key[0].reshape(d_model, kv_width), w_val[0].reshape(d_model, kv_width)], axis=1)

        hg = lax.ppermute(jnp.concatenate([h_dec[0], cot_out[0]], axis=1), 'stage', partner_perm)
        hid, cot = hg[:, :d_model], hg[:, d_model:]
        hg_all = gather(hg)
        hid_all, cot_all = hg_all[:, :d_model], hg_all[:, d_model:]
        s_dec = hid.shape[0]

        def heads_of(flat):
            return flat.reshape(s_dec, kv_heads, group, head).transpose(1, 2, 0, 3).reshape(kv_heads, group * s_dec, head)

        def flat_of(heads):
            return heads.reshape(kv_heads, group, s_dec, head).transpose(2, 0, 1, 3).reshape(s_dec, d_model)

        pre = dot(x, up, 1, 0)
        act, gelu_pull = jax.vjp(jax.nn.gelu, pre)
        act = act.astype(BF16)
        memory = (x.astype(F32) + dot(act, down, 1, 0)).astype(BF16)
        kv = dot(memory, w_kv, 1, 0).astype(BF16)
        kv_h = kv.reshape(-1, 2, kv_heads, head).transpose(1, 2, 0, 3)
        key_h, val_h = kv_h[0], kv_h[1]

        query = heads_of(dot(hid, w_q, 1, 0).astype(BF16))
        scale = head ** -0.5
        prob = jax.nn.softmax(bdot(query, key_h, 2, 2) * scale, axis=-1)
        prob_bf = prob.astype(BF16)
        ctx = flat_of(bdot(prob_bf, val_h, 2, 1).astype(BF16))
        mid = (hid.astype(F32) + dot(ctx, w_o, 1, 0)).astype(BF16)
        cm_all = gather(jnp.concatenate([ctx, mid], axis=1))
        ctx_all, mid_all = cm_all[:, :d_model], cm_all[:, d_model:]
        dec_act, dec_pull = jax.vjp(jax.nn.gelu, dot(mid, w_1, 1, 0))
        dec_act = dec_act.astype(BF16)
        dec_gact = dot(cot, w_2, 1, 1).astype(BF16)
        dec_gpre = dec_pull(dec_gact.astype(F32))[0].astype(BF16)
        g_mid = (cot.astype(F32) + dot(dec_gpre, w_1, 1, 1)).astype(BF16)
        g_ctx = heads_of(dot(g_mid, w_o, 1, 1).astype(BF16))
        g_prob = bdot(g_ctx, val_h, 2, 2)
        g_val = bdot(prob_bf, g_ctx, 1, 1).astype(BF16)
        g_logit = (prob * (g_prob - jnp.sum(prob * g_prob, axis=-1, keepdims=True)) * scale).astype(BF16)
        g_key = bdot(g_logit, query, 1, 1).astype(BF16)
        g_kv = jnp.concatenate([g_key[i] for i in range(kv_heads)] + [g_val[i] for i in range(kv_heads)], axis=1)
        g_mem = dot(g_kv, w_kv, 1, 1).astype(BF16)

        g_wkv = scatter(dot(memory, g_kv, 0, 0))
        g_down_own, g_mem, g_logit, g_mid, dec_gpre = lax.optimization_barrier((dot(act, g_mem, 0, 0), g_mem, g_logit, g_mid, dec_gpre))
        g_down = scatter(g_down_own)
        g_act = dot(g_mem, down, 1, 1).astype(BF16)
        g_pre = gelu_pull(g_act.astype(F32))[0].astype(BF16)
        g_up_own = with_layout_constraint(dot(x, g_pre, 0, 0), Layout((0, 1)))
        g_up_own, g_pre, g_logit, g_mid, dec_gpre = lax.optimization_barrier((g_up_own, g_pre, g_logit, g_mid, dec_gpre))
        g_up = scatter(g_up_own)

        g_query = flat_of(bdot(g_logit, key_h, 2, 1).astype(BF16))
        dh = (g_mid.astype(F32) + dot(g_query, w_q, 1, 1)).astype(BF16)
        dh = lax.ppermute(dh, 'stage', partner_perm)

        n1 = d_model // n_dev
        n2 = w_1.shape[1] // n_dev
        sent = [t.reshape(s_dec, n_dev, -1) for t in (dec_act, dec_gpre, g_mid, g_query)]
        cols = lax.all_to_all(jnp.concatenate(sent, axis=2), AXES, split_axis=1, concat_axis=0, tiled=True)
        cols = cols.reshape(n_dev * s_dec, -1)
        act_c, gpre_c, gmid_c, gq_c = (cols[:, :n2], cols[:, n2:2 * n2], cols[:, 2 * n2:2 * n2 + n1], cols[:, 2 * n2 + n1:])
        g_w2 = dot(act_c, cot_all, 0, 0)
        blocks = jnp.concatenate([dot(mid_all, gpre_c, 0, 0), dot(ctx_all, gmid_c, 0, 0), dot(hid_all, gq_c, 0, 0)], axis=1)
        blocks = lax.all_to_all(blocks.reshape(n_dev, n1, -1), AXES, split_axis=0, concat_axis=0, tiled=True)
        g_w1, g_wo, g_wq = (b.transpose(1, 0, 2).reshape(n1, -1) for b in (blocks[:, :, :n2], blocks[:, :, n2:n2 + n1], blocks[:, :, n2 + n1:]))
        dx = (g_mem.astype(F32) + dot(g_pre, up, 1, 1)).astype(BF16)
        g_wk = g_wkv[:, :kv_width].reshape(1, n1, kv_heads, head)
        g_wv = g_wkv[:, kv_width:].reshape(1, n1, kv_heads, head)
        return (dx[None], dh[None], g_up[None], g_down[None], g_wk, g_wv, g_wq[None], g_wo[None], g_w1[None], g_w2[None])

    return jax.shard_map(step, mesh=mesh,
                         in_specs=(row_spec, row_spec, row_spec, full_spec3, full_spec3, full_spec4, full_spec4, full_spec3, full_spec3, full_spec3, full_spec3),
                         out_specs=(row_spec, row_spec, grad_spec3, grad_spec3, grad_spec4, grad_spec4, grad_spec3, grad_spec3, grad_spec3, grad_spec3),
                         check_vma=False)
```

```python
import jax
import jax.numpy as jnp
from jax import lax
from jax.experimental.layout import Layout, with_layout_constraint
from jax.sharding import PartitionSpec as P


F32 = jnp.float32
BF16 = jnp.bfloat16
AXES = ('data', 'chip', 'core')
CHIPS = ('data', 'chip')


def dot(lhs, rhs, lhs_dim, rhs_dim):
    return lax.dot_general(lhs, rhs, (((lhs_dim,), (rhs_dim,)), ((), ())), preferred_element_type=F32)


def bdot(lhs, rhs, lhs_dim, rhs_dim):
    return lax.dot_general(lhs, rhs, (((lhs_dim,), (rhs_dim,)), ((0,), (0,))), preferred_element_type=F32)


def gather(rows):
    return lax.all_gather(rows, AXES, axis=0, tiled=True)


def scatter(own):
    return lax.psum_scatter(own, CHIPS, scatter_dimension=0, tiled=True)


def solution(mesh):
    n_data, chips = mesh.shape['data'], mesh.shape['stage'] // 2
    n_dev = n_data * chips * 2
    mesh = jax.sharding.Mesh(mesh.devices.reshape(n_data, chips, 2), AXES)
    partner_perm = [(index, (index + chips // 2) % chips) for index in range(chips)]
    row_spec = P(AXES, None, None)
    full_spec3 = P(None, None, None)
    full_spec4 = P(None, None, None, None)
    grad_spec3 = P(None, AXES, None)
    grad_spec4 = P(None, AXES, None, None)

    def step(x_enc, h_dec, cot_out, enc_up, enc_down, w_key, w_val, w_query, w_out, w_ff1, w_ff2):
        d_model = x_enc.shape[-1]
        kv_heads, head = w_key.shape[2], w_key.shape[3]
        group = d_model // (kv_heads * head)
        kv_width = kv_heads * head
        x, up, down = x_enc[0], enc_up[0], enc_down[0]
        w_q, w_o, w_1, w_2 = w_query[0], w_out[0], w_ff1[0], w_ff2[0]
        w_kv = jnp.concatenate([w_key[0].reshape(d_model, kv_width), w_val[0].reshape(d_model, kv_width)], axis=1)

        hg = lax.ppermute(jnp.concatenate([h_dec[0], cot_out[0]], axis=1), 'chip', partner_perm)
        hid, cot = hg[:, :d_model], hg[:, d_model:]
        hg_all = gather(hg)
        hid_all, cot_all = hg_all[:, :d_model], hg_all[:, d_model:]
        s_dec = hid.shape[0]

        def heads_of(flat):
            return flat.reshape(s_dec, kv_heads, group, head).transpose(1, 2, 0, 3).reshape(kv_heads, group * s_dec, head)

        def flat_of(heads):
            return heads.reshape(kv_heads, group, s_dec, head).transpose(2, 0, 1, 3).reshape(s_dec, d_model)

        core = lax.axis_index('core')

        def swap(own):
            return lax.ppermute(own, 'core', [(0, 1), (1, 0)])

        def half(arr, axis, index):
            size = arr.shape[axis] // 2
            return lax.dynamic_slice_in_dim(arr, index.astype(jnp.uint32) * size, size, axis)

        def join(own, other):
            return jnp.where(core == 0, jnp.concatenate([own, other], axis=1), jnp.concatenate([other, own], axis=1))

        x_sib = swap(x)
        pre = dot(x, up, 1, 0)
        act = lax.optimization_barrier(jax.nn.gelu(pre).astype(BF16))
        act_sib = swap(act)
        memory = (x.astype(F32) + dot(act, down, 1, 0)).astype(BF16)
        mem_sib = swap(memory)
        kv = dot(memory, w_kv, 1, 0).astype(BF16)
        kv_h = kv.reshape(-1, 2, kv_heads, head).transpose(1, 2, 0, 3)
        key_h, val_h = kv_h[0], kv_h[1]

        query = heads_of(dot(hid, w_q, 1, 0).astype(BF16))
        scale = head ** -0.5
        prob = jax.nn.softmax(bdot(query, key_h, 2, 2) * scale, axis=-1)
        prob_bf = prob.astype(BF16)
        ctx = flat_of(bdot(prob_bf, val_h, 2, 1).astype(BF16))
        mid = (hid.astype(F32) + dot(ctx, w_o, 1, 0)).astype(BF16)
        cm_all = gather(jnp.concatenate([ctx, mid], axis=1))
        ctx_all, mid_all = cm_all[:, :d_model], cm_all[:, d_model:]
        dec_act, dec_pull = jax.vjp(jax.nn.gelu, dot(mid, w_1, 1, 0))
        dec_act = dec_act.astype(BF16)
        dec_gact = dot(cot, w_2, 1, 1).astype(BF16)
        dec_gpre = dec_pull(dec_gact.astype(F32))[0].astype(BF16)
        gpre_all = gather(dec_gpre)
        g_mid = (cot.astype(F32) + dot(dec_gpre, w_1, 1, 1)).astype(BF16)
        g_ctx = heads_of(dot(g_mid, w_o, 1, 1).astype(BF16))
        g_prob = bdot(g_ctx, val_h, 2, 2)
        g_val = bdot(prob_bf, g_ctx, 1, 1).astype(BF16)
        g_logit = (prob * (g_prob - jnp.sum(prob * g_prob, axis=-1, keepdims=True)) * scale).astype(BF16)
        g_key = bdot(g_logit, query, 1, 1).astype(BF16)
        g_kv = jnp.concatenate([g_key[i] for i in range(kv_heads)] + [g_val[i] for i in range(kv_heads)], axis=1)
        g_mem = dot(g_kv, w_kv, 1, 1).astype(BF16)

        kv_sib = swap(g_kv)
        gm_sib = dot(kv_sib, half(w_kv, 0, core), 1, 1).astype(BF16)
        own = lax.optimization_barrier(dot(act, half(g_mem, 1, core), 0, 0))
        down_half = own + dot(act_sib, gm_sib, 0, 0)
        down_half, g_mem, g_logit, g_mid, dec_gpre, kv_sib, mem_sib = lax.optimization_barrier((down_half, g_mem, g_logit, g_mid, dec_gpre, kv_sib, mem_sib))
        down_sum = scatter(down_half)

        def gpre_half(index):
            g_act = dot(g_mem, half(down, 0, index), 1, 1).astype(BF16)
            return jax.vjp(jax.nn.gelu, half(pre, 1, index))[1](g_act.astype(F32))[0].astype(BF16)

        gpre_send = gpre_half(1 - core)
        gpre_sib = swap(gpre_send)
        gpre_own = gpre_half(core)
        wkv_half = dot(memory, half(g_kv, 1, core), 0, 0) + dot(mem_sib, half(kv_sib, 1, core), 0, 0)
        own = lax.optimization_barrier(dot(x, gpre_own, 0, 0))
        up_half = with_layout_constraint(own + dot(x_sib, gpre_sib, 0, 0), Layout((0, 1)))
        up_half = with_layout_constraint(jnp.concatenate([up_half, wkv_half], axis=1), Layout((0, 1)))
        up_half, gpre_own, g_logit, g_mid, dec_gpre = lax.optimization_barrier((up_half, gpre_own, g_logit, g_mid, dec_gpre))
        up_sum = scatter(up_half)
        n1 = d_model // n_dev
        n2 = w_1.shape[1] // n_dev
        g_down = join(half(down_sum, 0, core), swap(half(down_sum, 0, 1 - core)))
        up_own, up_other = half(up_sum, 0, core), swap(half(up_sum, 0, 1 - core))
        n_ff = up_own.shape[1] - kv_width
        g_up = join(up_own[:, :n_ff], up_other[:, :n_ff])
        g_wkv = join(up_own[:, n_ff:], up_other[:, n_ff:])

        g_query = flat_of(bdot(g_logit, key_h, 2, 1).astype(BF16))
        dh = (g_mid.astype(F32) + dot(g_query, w_q, 1, 1)).astype(BF16)
        dh = lax.ppermute(dh, 'chip', partner_perm)

        sent = [t.reshape(s_dec, n_dev, -1) for t in (dec_act, g_mid, g_query)]
        cols = lax.all_to_all(jnp.concatenate(sent, axis=2), AXES, split_axis=1, concat_axis=0, tiled=True)
        cols = cols.reshape(n_dev * s_dec, -1)
        act_c, gmid_c, gq_c = cols[:, :n2], cols[:, n2:n2 + n1], cols[:, n2 + n1:]
        g_w2 = dot(act_c, cot_all, 0, 0)
        mid_c = lax.dynamic_slice_in_dim(mid_all, lax.axis_index(AXES) * n1, n1, 1)
        g_w1 = dot(mid_c, gpre_all, 0, 0)
        blocks = jnp.concatenate([dot(ctx_all, gmid_c, 0, 0), dot(hid_all, gq_c, 0, 0)], axis=1)
        blocks = lax.all_to_all(blocks.reshape(n_dev, n1, -1), AXES, split_axis=0, concat_axis=0, tiled=True)
        g_wo, g_wq = (b.transpose(1, 0, 2).reshape(n1, -1) for b in (blocks[:, :, :n1], blocks[:, :, n1:]))
        part = lax.optimization_barrier(dot(gpre_own, half(up, 1, core), 1, 1))
        dx = (g_mem.astype(F32) + part + dot(gpre_send, half(up, 1, 1 - core), 1, 1)).astype(BF16)
        g_wk = g_wkv[:, :kv_width].reshape(1, n1, kv_heads, head)
        g_wv = g_wkv[:, kv_width:].reshape(1, n1, kv_heads, head)
        return (dx[None], dh[None], g_up[None], g_down[None], g_wk, g_wv, g_wq[None], g_wo[None], g_w1[None], g_w2[None])

    return jax.shard_map(step, mesh=mesh,
                         in_specs=(row_spec, row_spec, row_spec, full_spec3, full_spec3, full_spec4, full_spec4, full_spec3, full_spec3, full_spec3, full_spec3),
                         out_specs=(row_spec, row_spec, grad_spec3, grad_spec3, grad_spec4, grad_spec4, grad_spec3, grad_spec3, grad_spec3, grad_spec3),
                         check_vma=False)
```

```python
import jax
import jax.numpy as jnp
from jax import lax
from jax.experimental import pallas as pl
from jax.experimental.pallas import tpu as pltpu
from jax.experimental.layout import Layout, with_layout_constraint
from jax.sharding import PartitionSpec as P


F32 = jnp.float32
BF16 = jnp.bfloat16
AXES = ('data', 'chip', 'core')
CHIPS = ('data', 'chip')


def dot(lhs, rhs, lhs_dim, rhs_dim):
    return lax.dot_general(lhs, rhs, (((lhs_dim,), (rhs_dim,)), ((), ())), preferred_element_type=F32)


def bdot(lhs, rhs, lhs_dim, rhs_dim):
    return lax.dot_general(lhs, rhs, (((lhs_dim,), (rhs_dim,)), ((0,), (0,))), preferred_element_type=F32)


def gather(rows):
    return lax.all_gather(rows, AXES, axis=0, tiled=True)


def scatter(own):
    return lax.psum_scatter(own, CHIPS, scatter_dimension=0, tiled=True)


def dec_mlp_kernel(mid_ref, cot_ref, w1_ref, w2_ref, act_ref, gpre_ref, gmid_ref, acc_ref):
    @pl.when(pl.program_id(0) == 0)
    def _():
        acc_ref[...] = jnp.zeros_like(acc_ref)

    act, gelu_pull = jax.vjp(jax.nn.gelu, dot(mid_ref[...], w1_ref[...], 1, 0))
    act_ref[...] = act.astype(BF16)
    g_act = dot(w2_ref[...], cot_ref[...], 1, 1).T.astype(BF16)
    g_pre = gelu_pull(g_act.astype(F32))[0].astype(BF16)
    gpre_ref[...] = g_pre
    acc_ref[...] += dot(w1_ref[...], g_pre, 1, 1)

    @pl.when(pl.program_id(0) == pl.num_programs(0) - 1)
    def _():
        gmid_ref[...] = (cot_ref[...].astype(F32) + acc_ref[...].T).astype(BF16)


def dec_mlp(mid, cot, w_1, w_2, block):
    s_dec, d_model = mid.shape
    width = w_1.shape[1]
    rows = pl.BlockSpec((s_dec, d_model), lambda i: (0, 0))
    cols = pl.BlockSpec((s_dec, block), lambda i: (0, i))
    return pl.pallas_call(
        dec_mlp_kernel,
        grid=(width // block,),
        in_specs=[rows, rows, pl.BlockSpec((d_model, block), lambda i: (0, i)), pl.BlockSpec((block, d_model), lambda i: (i, 0))],
        out_specs=[cols, cols, rows],
        out_shape=[jax.ShapeDtypeStruct((s_dec, width), BF16)] * 2 + [jax.ShapeDtypeStruct((s_dec, d_model), BF16)],
        scratch_shapes=[pltpu.VMEM((d_model, s_dec), F32)],
        compiler_params=pltpu.CompilerParams(dimension_semantics=('arbitrary',), vmem_limit_bytes=32 * 2 ** 20),
        cost_estimate=pl.CostEstimate(flops=6 * s_dec * d_model * width, bytes_accessed=4 * d_model * width, transcendentals=s_dec * width),
    )(mid, cot, w_1, w_2)


def solution(mesh):
    n_data, chips = mesh.shape['data'], mesh.shape['stage'] // 2
    n_dev = n_data * chips * 2
    mesh = jax.sharding.Mesh(mesh.devices.reshape(n_data, chips, 2), AXES)
    partner_perm = [(index, (index + chips // 2) % chips) for index in range(chips)]
    row_spec = P(AXES, None, None)
    full_spec3 = P(None, None, None)
    full_spec4 = P(None, None, None, None)
    grad_spec3 = P(None, AXES, None)
    grad_spec4 = P(None, AXES, None, None)

    def step(x_enc, h_dec, cot_out, enc_up, enc_down, w_key, w_val, w_query, w_out, w_ff1, w_ff2):
        d_model = x_enc.shape[-1]
        kv_heads, head = w_key.shape[2], w_key.shape[3]
        group = d_model // (kv_heads * head)
        kv_width = kv_heads * head
        x, up, down = x_enc[0], enc_up[0], enc_down[0]
        w_q, w_o, w_1, w_2 = w_query[0], w_out[0], w_ff1[0], w_ff2[0]
        w_kv = jnp.concatenate([w_key[0].reshape(d_model, kv_width), w_val[0].reshape(d_model, kv_width)], axis=1)

        hg_own = jnp.concatenate([h_dec[0], cot_out[0]], axis=1)
        hg = lax.ppermute(hg_own, 'chip', partner_perm)
        hid, cot = hg[:, :d_model], hg[:, d_model:]
        hg_all = gather(hg_own)
        hid_all, cot_all = hg_all[:, :d_model], hg_all[:, d_model:]
        s_dec = hid.shape[0]

        def heads_of(flat):
            return flat.reshape(s_dec, kv_heads, group, head).transpose(1, 2, 0, 3).reshape(kv_heads, group * s_dec, head)

        def flat_of(heads):
            return heads.reshape(kv_heads, group, s_dec, head).transpose(2, 0, 1, 3).reshape(s_dec, d_model)

        core = lax.axis_index('core')

        def swap(own):
            return lax.ppermute(own, 'core', [(0, 1), (1, 0)])

        def half(arr, axis, index):
            size = arr.shape[axis] // 2
            return lax.dynamic_slice_in_dim(arr, index.astype(jnp.uint32) * size, size, axis)

        def join(own, other):
            return jnp.where(core == 0, jnp.concatenate([own, other], axis=1), jnp.concatenate([other, own], axis=1))

        x_sib = swap(x)
        pre = dot(x, up, 1, 0)
        act = lax.optimization_barrier(jax.nn.gelu(pre).astype(BF16))
        act_sib = swap(act)
        memory = (x.astype(F32) + dot(act, down, 1, 0)).astype(BF16)
        mem_sib = swap(memory)
        kv = dot(memory, w_kv, 1, 0).astype(BF16)
        kv_h = kv.reshape(-1, 2, kv_heads, head).transpose(1, 2, 0, 3)
        key_h, val_h = kv_h[0], kv_h[1]

        query = heads_of(dot(hid, w_q, 1, 0).astype(BF16))
        scale = head ** -0.5
        prob = jax.nn.softmax(bdot(query, key_h, 2, 2) * scale, axis=-1)
        prob_bf = prob.astype(BF16)
        ctx = flat_of(bdot(prob_bf, val_h, 2, 1).astype(BF16))
        mid = (hid.astype(F32) + dot(ctx, w_o, 1, 0)).astype(BF16)
        cm_all = gather(jnp.concatenate([ctx, mid], axis=1))
        ctx_all, mid_all = cm_all[:, :d_model], cm_all[:, d_model:]
        dec_act, dec_gpre, g_mid = dec_mlp(mid, cot, w_1, w_2, w_1.shape[1] // 10)
        gpre_all = gather(dec_gpre)
        g_ctx = heads_of(dot(g_mid, w_o, 1, 1).astype(BF16))
        g_prob = bdot(g_ctx, val_h, 2, 2)
        g_val = bdot(prob_bf, g_ctx, 1, 1).astype(BF16)
        g_logit = (prob * (g_prob - jnp.sum(prob * g_prob, axis=-1, keepdims=True)) * scale).astype(BF16)
        g_key = bdot(g_logit, query, 1, 1).astype(BF16)
        g_kv = jnp.concatenate([g_key[i] for i in range(kv_heads)] + [g_val[i] for i in range(kv_heads)], axis=1)
        g_mem = dot(g_kv, w_kv, 1, 1).astype(BF16)

        kv_sib = swap(g_kv)
        gm_sib = dot(kv_sib, half(w_kv, 0, core), 1, 1).astype(BF16)
        own = lax.optimization_barrier(dot(act, half(g_mem, 1, core), 0, 0))
        down_half = own + dot(act_sib, gm_sib, 0, 0)
        down_half, g_mem, g_logit, g_mid, dec_gpre, kv_sib, mem_sib = lax.optimization_barrier((down_half, g_mem, g_logit, g_mid, dec_gpre, kv_sib, mem_sib))
        down_sum = scatter(down_half)

        def gpre_half(index):
            g_act = dot(g_mem, half(down, 0, index), 1, 1).astype(BF16)
            return jax.vjp(jax.nn.gelu, half(pre, 1, index))[1](g_act.astype(F32))[0].astype(BF16)

        gpre_send = gpre_half(1 - core)
        gpre_sib = swap(gpre_send)
        gpre_own = gpre_half(core)
        wkv_half = dot(memory, half(g_kv, 1, core), 0, 0) + dot(mem_sib, half(kv_sib, 1, core), 0, 0)
        own = lax.optimization_barrier(dot(x, gpre_own, 0, 0))
        up_half = with_layout_constraint(own + dot(x_sib, gpre_sib, 0, 0), Layout((0, 1)))
        up_half = with_layout_constraint(jnp.concatenate([up_half, wkv_half], axis=1), Layout((0, 1)))
        up_half, gpre_own, g_logit, g_mid, dec_gpre = lax.optimization_barrier((up_half, gpre_own, g_logit, g_mid, dec_gpre))
        up_sum = scatter(up_half)
        n1 = d_model // n_dev
        n2 = w_1.shape[1] // n_dev
        g_down = join(half(down_sum, 0, core), swap(half(down_sum, 0, 1 - core)))
        up_own, up_other = half(up_sum, 0, core), swap(half(up_sum, 0, 1 - core))
        n_ff = up_own.shape[1] - kv_width
        g_up = join(up_own[:, :n_ff], up_other[:, :n_ff])
        g_wkv = join(up_own[:, n_ff:], up_other[:, n_ff:])

        g_query = flat_of(bdot(g_logit, key_h, 2, 1).astype(BF16))
        dh = (g_mid.astype(F32) + dot(g_query, w_q, 1, 1)).astype(BF16)
        dh = lax.ppermute(dh, 'chip', partner_perm)

        sent = [t.reshape(s_dec, n_dev, -1) for t in (dec_act, g_mid, g_query)]
        cols = lax.all_to_all(jnp.concatenate(sent, axis=2), AXES, split_axis=1, concat_axis=0, tiled=True)
        cols = cols.reshape(n_dev * s_dec, -1)
        gmid_c = cols[:, n2:n2 + n1]
        halves = cols.reshape(n_data, 2, chips // 2, 2 * s_dec, -1)
        cols = jnp.concatenate([halves[:, 1:], halves[:, :1]], axis=1).reshape(n_dev * s_dec, -1)
        act_c, gq_c = cols[:, :n2], cols[:, n2 + n1:]
        g_w2 = dot(act_c, cot_all, 0, 0)
        mid_c = lax.dynamic_slice_in_dim(mid_all, lax.axis_index(AXES) * n1, n1, 1)
        g_w1 = dot(mid_c, gpre_all, 0, 0)
        blocks = jnp.concatenate([dot(ctx_all, gmid_c, 0, 0), dot(hid_all, gq_c, 0, 0)], axis=1)
        blocks = lax.all_to_all(blocks.reshape(n_dev, n1, -1), AXES, split_axis=0, concat_axis=0, tiled=True)
        g_wo, g_wq = (b.transpose(1, 0, 2).reshape(n1, -1) for b in (blocks[:, :, :n1], blocks[:, :, n1:]))
        part = lax.optimization_barrier(dot(gpre_own, half(up, 1, core), 1, 1))
        dx = (g_mem.astype(F32) + part + dot(gpre_send, half(up, 1, 1 - core), 1, 1)).astype(BF16)
        g_wk = g_wkv[:, :kv_width].reshape(1, n1, kv_heads, head)
        g_wv = g_wkv[:, kv_width:].reshape(1, n1, kv_heads, head)
        return (dx[None], dh[None], g_up[None], g_down[None], g_wk, g_wv, g_wq[None], g_wo[None], g_w1[None], g_w2[None])

    return jax.shard_map(step, mesh=mesh,
                         in_specs=(row_spec, row_spec, row_spec, full_spec3, full_spec3, full_spec4, full_spec4, full_spec3, full_spec3, full_spec3, full_spec3),
                         out_specs=(row_spec, row_spec, grad_spec3, grad_spec3, grad_spec4, grad_spec4, grad_spec3, grad_spec3, grad_spec3, grad_spec3),
                         check_vma=False)
```

```python
import functools

import jax
import jax.numpy as jnp
from jax import lax
from jax.experimental import pallas as pl
from jax.experimental.pallas import tpu as pltpu
from jax.experimental.layout import Layout, with_layout_constraint
from jax.sharding import PartitionSpec as P


F32 = jnp.float32
BF16 = jnp.bfloat16
AXES = ('data', 'chip', 'core')
CHIPS = ('data', 'chip')


def dot(lhs, rhs, lhs_dim, rhs_dim):
    return lax.dot_general(lhs, rhs, (((lhs_dim,), (rhs_dim,)), ((), ())), preferred_element_type=F32)


def bdot(lhs, rhs, lhs_dim, rhs_dim):
    return lax.dot_general(lhs, rhs, (((lhs_dim,), (rhs_dim,)), ((0,), (0,))), preferred_element_type=F32)


def gather(rows):
    return lax.all_gather(rows, AXES, axis=0, tiled=True)


def scatter(own):
    return lax.psum_scatter(own, CHIPS, scatter_dimension=0, tiled=True)


def dec_mlp_kernel(mid_ref, cot_ref, w1_ref, w2_ref, act_ref, gpre_ref, gmid_ref, acc_ref):
    @pl.when(pl.program_id(0) == 0)
    def _():
        acc_ref[...] = jnp.zeros_like(acc_ref)

    act, gelu_pull = jax.vjp(jax.nn.gelu, dot(mid_ref[...], w1_ref[...], 1, 0))
    act_ref[...] = act.astype(BF16)
    g_act = dot(w2_ref[...], cot_ref[...], 1, 1).T.astype(BF16)
    g_pre = gelu_pull(g_act.astype(F32))[0].astype(BF16)
    gpre_ref[...] = g_pre
    acc_ref[...] += dot(w1_ref[...], g_pre, 1, 1)

    @pl.when(pl.program_id(0) == pl.num_programs(0) - 1)
    def _():
        gmid_ref[...] = (cot_ref[...].astype(F32) + acc_ref[...].T).astype(BF16)


def dec_mlp(mid, cot, w_1, w_2, block):
    s_dec, d_model = mid.shape
    width = w_1.shape[1]
    rows = pl.BlockSpec((s_dec, d_model), lambda i: (0, 0))
    cols = pl.BlockSpec((s_dec, block), lambda i: (0, i))
    return pl.pallas_call(
        dec_mlp_kernel,
        grid=(width // block,),
        in_specs=[rows, rows, pl.BlockSpec((d_model, block), lambda i: (0, i)), pl.BlockSpec((block, d_model), lambda i: (i, 0))],
        out_specs=[cols, cols, rows],
        out_shape=[jax.ShapeDtypeStruct((s_dec, width), BF16)] * 2 + [jax.ShapeDtypeStruct((s_dec, d_model), BF16)],
        scratch_shapes=[pltpu.VMEM((d_model, s_dec), F32)],
        compiler_params=pltpu.CompilerParams(dimension_semantics=('arbitrary',), vmem_limit_bytes=32 * 2 ** 20),
        cost_estimate=pl.CostEstimate(flops=6 * s_dec * d_model * width, bytes_accessed=4 * d_model * width, transcendentals=s_dec * width),
    )(mid, cot, w_1, w_2)


def enc_mlp_kernel(rows, x_ref, up_ref, down_ref, pre_ref, act_ref, mem_ref, acc_ref):
    step = pl.program_id(0)

    @pl.when(step == 0)
    def _():
        acc_ref[...] = jnp.zeros_like(acc_ref)

    @pl.loop(0, x_ref.shape[0] // rows)
    def _(i):
        part = pl.ds(pl.multiple_of(i * rows, rows), rows)
        pre = dot(x_ref[part, :], up_ref[...], 1, 0)
        pre_ref[part, :] = pre
        act_ref[part, :] = jax.nn.gelu(pre).astype(BF16)
        acc_ref[part, :] += dot(act_ref[part, :], down_ref[...], 1, 0)

    @pl.when(step == pl.num_programs(0) - 1)
    def _():
        mem_ref[...] = (x_ref[...].astype(F32) + acc_ref[...]).astype(BF16)


def enc_mlp(x, up, down, block, rows):
    seq, d_model = x.shape
    width = up.shape[1]
    full = pl.BlockSpec((seq, d_model), lambda i: (0, 0), pipeline_mode=pl.Buffered(1))
    cols = pl.BlockSpec((seq, block), lambda i: (0, i))
    return pl.pallas_call(
        functools.partial(enc_mlp_kernel, rows),
        grid=(width // block,),
        in_specs=[full, pl.BlockSpec((d_model, block), lambda i: (0, i)), pl.BlockSpec((block, d_model), lambda i: (i, 0))],
        out_specs=[cols, cols, full],
        out_shape=[jax.ShapeDtypeStruct((seq, width), F32), jax.ShapeDtypeStruct((seq, width), BF16), jax.ShapeDtypeStruct((seq, d_model), BF16)],
        scratch_shapes=[pltpu.VMEM((seq, d_model), F32)],
        compiler_params=pltpu.CompilerParams(dimension_semantics=('arbitrary',), vmem_limit_bytes=63 * 2 ** 20),
        cost_estimate=pl.CostEstimate(flops=4 * seq * d_model * width, bytes_accessed=4 * d_model * width + 6 * seq * width, transcendentals=seq * width),
    )(x, up, down)


def solution(mesh):
    n_data, chips = mesh.shape['data'], mesh.shape['stage'] // 2
    n_dev = n_data * chips * 2
    mesh = jax.sharding.Mesh(mesh.devices.reshape(n_data, chips, 2), AXES)
    partner_perm = [(index, (index + chips // 2) % chips) for index in range(chips)]
    row_spec = P(AXES, None, None)
    full_spec3 = P(None, None, None)
    full_spec4 = P(None, None, None, None)
    grad_spec3 = P(None, AXES, None)
    grad_spec4 = P(None, AXES, None, None)

    def step(x_enc, h_dec, cot_out, enc_up, enc_down, w_key, w_val, w_query, w_out, w_ff1, w_ff2):
        d_model = x_enc.shape[-1]
        kv_heads, head = w_key.shape[2], w_key.shape[3]
        group = d_model // (kv_heads * head)
        kv_width = kv_heads * head
        x, up, down = x_enc[0], enc_up[0], enc_down[0]
        w_q, w_o, w_1, w_2 = w_query[0], w_out[0], w_ff1[0], w_ff2[0]
        w_kv = jnp.concatenate([w_key[0].reshape(d_model, kv_width), w_val[0].reshape(d_model, kv_width)], axis=1)

        hg_own = jnp.concatenate([h_dec[0], cot_out[0]], axis=1)
        hg = lax.ppermute(hg_own, 'chip', partner_perm)
        hid, cot = hg[:, :d_model], hg[:, d_model:]
        hg_all = gather(hg_own)
        hid_all, cot_all = hg_all[:, :d_model], hg_all[:, d_model:]
        s_dec = hid.shape[0]

        def heads_of(flat):
            return flat.reshape(s_dec, kv_heads, group, head).transpose(1, 2, 0, 3).reshape(kv_heads, group * s_dec, head)

        def flat_of(heads):
            return heads.reshape(kv_heads, group, s_dec, head).transpose(2, 0, 1, 3).reshape(s_dec, d_model)

        core = lax.axis_index('core')

        def swap(own):
            return lax.ppermute(own, 'core', [(0, 1), (1, 0)])

        def half(arr, axis, index):
            size = arr.shape[axis] // 2
            return lax.dynamic_slice_in_dim(arr, index.astype(jnp.uint32) * size, size, axis)

        def join(own, other):
            return jnp.where(core == 0, jnp.concatenate([own, other], axis=1), jnp.concatenate([other, own], axis=1))

        x_sib = swap(x)
        pre, act, memory = enc_mlp(x, up, down, up.shape[1] // 7, x.shape[0] // 3)
        act_sib = swap(act)
        mem_sib = swap(memory)
        kv = dot(memory, w_kv, 1, 0).astype(BF16)
        kv_h = kv.reshape(-1, 2, kv_heads, head).transpose(1, 2, 0, 3)
        key_h, val_h = kv_h[0], kv_h[1]

        query = heads_of(dot(hid, w_q, 1, 0).astype(BF16))
        scale = head ** -0.5
        prob = jax.nn.softmax(bdot(query, key_h, 2, 2) * scale, axis=-1)
        prob_bf = prob.astype(BF16)
        ctx = flat_of(bdot(prob_bf, val_h, 2, 1).astype(BF16))
        mid = (hid.astype(F32) + dot(ctx, w_o, 1, 0)).astype(BF16)
        cm_all = gather(jnp.concatenate([ctx, mid], axis=1))
        ctx_all, mid_all = cm_all[:, :d_model], cm_all[:, d_model:]
        dec_act, dec_gpre, g_mid = dec_mlp(mid, cot, w_1, w_2, w_1.shape[1] // 7)
        gpre_all = gather(dec_gpre)
        g_ctx = heads_of(dot(g_mid, w_o, 1, 1).astype(BF16))
        g_prob = bdot(g_ctx, val_h, 2, 2)
        g_val = bdot(prob_bf, g_ctx, 1, 1).astype(BF16)
        g_logit = (prob * (g_prob - jnp.sum(prob * g_prob, axis=-1, keepdims=True)) * scale).astype(BF16)
        g_key = bdot(g_logit, query, 1, 1).astype(BF16)
        g_kv = jnp.concatenate([g_key[i] for i in range(kv_heads)] + [g_val[i] for i in range(kv_heads)], axis=1)
        g_mem = dot(g_kv, w_kv, 1, 1).astype(BF16)

        kv_sib = swap(g_kv)
        gm_sib = dot(kv_sib, half(w_kv, 0, core), 1, 1).astype(BF16)
        own = lax.optimization_barrier(dot(act, half(g_mem, 1, core), 0, 0))
        down_half = own + dot(act_sib, gm_sib, 0, 0)
        down_half, g_mem, g_logit, g_mid, dec_gpre, kv_sib, mem_sib = lax.optimization_barrier((down_half, g_mem, g_logit, g_mid, dec_gpre, kv_sib, mem_sib))
        down_sum = scatter(down_half)

        def gpre_half(index):
            g_act = dot(g_mem, half(down, 0, index), 1, 1).astype(BF16)
            return jax.vjp(jax.nn.gelu, half(pre, 1, index))[1](g_act.astype(F32))[0].astype(BF16)

        gpre_send = gpre_half(1 - core)
        gpre_sib = swap(gpre_send)
        gpre_own = gpre_half(core)
        wkv_half = dot(memory, half(g_kv, 1, core), 0, 0) + dot(mem_sib, half(kv_sib, 1, core), 0, 0)
        own = lax.optimization_barrier(dot(x, gpre_own, 0, 0))
        up_half = with_layout_constraint(own + dot(x_sib, gpre_sib, 0, 0), Layout((0, 1)))
        up_half = with_layout_constraint(jnp.concatenate([up_half, wkv_half], axis=1), Layout((0, 1)))
        up_half, gpre_own, g_logit, g_mid, dec_gpre = lax.optimization_barrier((up_half, gpre_own, g_logit, g_mid, dec_gpre))
        up_sum = scatter(up_half)
        n1 = d_model // n_dev
        n2 = w_1.shape[1] // n_dev
        g_down = join(half(down_sum, 0, core), swap(half(down_sum, 0, 1 - core)))
        up_own, up_other = half(up_sum, 0, core), swap(half(up_sum, 0, 1 - core))
        n_ff = up_own.shape[1] - kv_width
        g_up = join(up_own[:, :n_ff], up_other[:, :n_ff])
        g_wkv = join(up_own[:, n_ff:], up_other[:, n_ff:])

        g_query = flat_of(bdot(g_logit, key_h, 2, 1).astype(BF16))
        dh = (g_mid.astype(F32) + dot(g_query, w_q, 1, 1)).astype(BF16)
        dh = lax.ppermute(dh, 'chip', partner_perm)

        sent = [t.reshape(s_dec, n_dev, -1) for t in (dec_act, g_mid, g_query)]
        cols = lax.all_to_all(jnp.concatenate(sent, axis=2), AXES, split_axis=1, concat_axis=0, tiled=True)
        cols = cols.reshape(n_dev * s_dec, -1)
        gmid_c = cols[:, n2:n2 + n1]
        halves = cols.reshape(n_data, 2, chips // 2, 2 * s_dec, -1)
        cols = jnp.concatenate([halves[:, 1:], halves[:, :1]], axis=1).reshape(n_dev * s_dec, -1)
        act_c, gq_c = cols[:, :n2], cols[:, n2 + n1:]
        g_w2 = dot(act_c, cot_all, 0, 0)
        mid_c = lax.dynamic_slice_in_dim(mid_all, lax.axis_index(AXES) * n1, n1, 1)
        g_w1 = dot(mid_c, gpre_all, 0, 0)
        blocks = jnp.concatenate([dot(ctx_all, gmid_c, 0, 0), dot(hid_all, gq_c, 0, 0)], axis=1)
        blocks = lax.all_to_all(blocks.reshape(n_dev, n1, -1), AXES, split_axis=0, concat_axis=0, tiled=True)
        g_wo, g_wq = (b.transpose(1, 0, 2).reshape(n1, -1) for b in (blocks[:, :, :n1], blocks[:, :, n1:]))
        part = lax.optimization_barrier(dot(gpre_own, half(up, 1, core), 1, 1))
        dx = (g_mem.astype(F32) + part + dot(gpre_send, half(up, 1, 1 - core), 1, 1)).astype(BF16)
        g_wk = g_wkv[:, :kv_width].reshape(1, n1, kv_heads, head)
        g_wv = g_wkv[:, kv_width:].reshape(1, n1, kv_heads, head)
        return (dx[None], dh[None], g_up[None], g_down[None], g_wk, g_wv, g_wq[None], g_wo[None], g_w1[None], g_w2[None])

    return jax.shard_map(step, mesh=mesh,
                         in_specs=(row_spec, row_spec, row_spec, full_spec3, full_spec3, full_spec4, full_spec4, full_spec3, full_spec3, full_spec3, full_spec3),
                         out_specs=(row_spec, row_spec, grad_spec3, grad_spec3, grad_spec4, grad_spec4, grad_spec3, grad_spec3, grad_spec3, grad_spec3),
                         check_vma=False)
```

```python
import jax
import jax.numpy as jnp
from jax import lax
from jax.experimental import pallas as pl
from jax.experimental.pallas import tpu as pltpu
from jax.experimental.layout import Layout, with_layout_constraint
from jax.sharding import PartitionSpec as P


F32 = jnp.float32
BF16 = jnp.bfloat16
AXES = ('data', 'chip', 'core')
CHIPS = ('data', 'chip')


def dot(lhs, rhs, lhs_dim, rhs_dim):
    return lax.dot_general(lhs, rhs, (((lhs_dim,), (rhs_dim,)), ((), ())), preferred_element_type=F32)


def bdot(lhs, rhs, lhs_dim, rhs_dim):
    return lax.dot_general(lhs, rhs, (((lhs_dim,), (rhs_dim,)), ((0,), (0,))), preferred_element_type=F32)


def gather(rows):
    return lax.all_gather(rows, AXES, axis=0, tiled=True)


def scatter(own):
    return lax.psum_scatter(own, CHIPS, scatter_dimension=0, tiled=True)


def dec_mlp_kernel(mid_ref, cot_ref, w1_ref, w2_ref, act_ref, gpre_ref, gmid_ref, acc_ref):
    @pl.when(pl.program_id(0) == 0)
    def _():
        acc_ref[...] = jnp.zeros_like(acc_ref)

    act, gelu_pull = jax.vjp(jax.nn.gelu, dot(mid_ref[...], w1_ref[...], 1, 0))
    act_ref[...] = act.astype(BF16)
    g_act = dot(w2_ref[...], cot_ref[...], 1, 1).T.astype(BF16)
    g_pre = gelu_pull(g_act.astype(F32))[0].astype(BF16)
    gpre_ref[...] = g_pre
    acc_ref[...] += dot(w1_ref[...], g_pre, 1, 1)

    @pl.when(pl.program_id(0) == pl.num_programs(0) - 1)
    def _():
        gmid_ref[...] = (cot_ref[...].astype(F32) + acc_ref[...].T).astype(BF16)


def dec_mlp(mid, cot, w_1, w_2, block):
    s_dec, d_model = mid.shape
    width = w_1.shape[1]
    rows = pl.BlockSpec((s_dec, d_model), lambda i: (0, 0))
    cols = pl.BlockSpec((s_dec, block), lambda i: (0, i))
    return pl.pallas_call(
        dec_mlp_kernel,
        grid=(width // block,),
        in_specs=[rows, rows, pl.BlockSpec((d_model, block), lambda i: (0, i)), pl.BlockSpec((block, d_model), lambda i: (i, 0))],
        out_specs=[cols, cols, rows],
        out_shape=[jax.ShapeDtypeStruct((s_dec, width), BF16)] * 2 + [jax.ShapeDtypeStruct((s_dec, d_model), BF16)],
        scratch_shapes=[pltpu.VMEM((d_model, s_dec), F32)],
        compiler_params=pltpu.CompilerParams(dimension_semantics=('arbitrary',), vmem_limit_bytes=32 * 2 ** 20),
        cost_estimate=pl.CostEstimate(flops=6 * s_dec * d_model * width, bytes_accessed=4 * d_model * width, transcendentals=s_dec * width),
    )(mid, cot, w_1, w_2)


def solution(mesh):
    n_data, chips = mesh.shape['data'], mesh.shape['stage'] // 2
    n_dev = n_data * chips * 2
    mesh = jax.sharding.Mesh(mesh.devices.reshape(n_data, chips, 2), AXES)
    partner_perm = [(index, (index + chips // 2) % chips) for index in range(chips)]
    row_spec = P(AXES, None, None)
    full_spec3 = P(None, None, None)
    full_spec4 = P(None, None, None, None)
    grad_spec3 = P(None, AXES, None)
    grad_spec4 = P(None, AXES, None, None)

    def step(x_enc, h_dec, cot_out, enc_up, enc_down, w_key, w_val, w_query, w_out, w_ff1, w_ff2):
        d_model = x_enc.shape[-1]
        kv_heads, head = w_key.shape[2], w_key.shape[3]
        group = d_model // (kv_heads * head)
        kv_width = kv_heads * head
        x, up, down = x_enc[0], enc_up[0], enc_down[0]
        w_q, w_o, w_1, w_2 = w_query[0], w_out[0], w_ff1[0], w_ff2[0]
        w_kv = jnp.concatenate([w_key[0].reshape(d_model, kv_width), w_val[0].reshape(d_model, kv_width)], axis=1)

        hg_own = jnp.concatenate([h_dec[0], cot_out[0]], axis=1)
        hg = lax.ppermute(hg_own, 'chip', partner_perm)
        hid, cot = hg[:, :d_model], hg[:, d_model:]
        hg_all = gather(hg_own)
        hid_all, cot_all = hg_all[:, :d_model], hg_all[:, d_model:]
        s_dec = hid.shape[0]

        def heads_of(flat):
            return flat.reshape(s_dec, kv_heads, group, head).transpose(1, 2, 0, 3).reshape(kv_heads, group * s_dec, head)

        def flat_of(heads):
            return heads.reshape(kv_heads, group, s_dec, head).transpose(2, 0, 1, 3).reshape(s_dec, d_model)

        core = lax.axis_index('core')

        def swap(own):
            return lax.ppermute(own, 'core', [(0, 1), (1, 0)])

        def half(arr, axis, index):
            size = arr.shape[axis] // 2
            return lax.dynamic_slice_in_dim(arr, index.astype(jnp.uint32) * size, size, axis)

        def join(own, other):
            return jnp.where(core == 0, jnp.concatenate([own, other], axis=1), jnp.concatenate([other, own], axis=1))

        x_sib = swap(x)
        pre = dot(x, up, 1, 0)
        act = lax.optimization_barrier(jax.nn.gelu(pre).astype(BF16))
        act_sib = swap(act)
        memory = (x.astype(F32) + dot(act, down, 1, 0)).astype(BF16)
        mem_sib = swap(memory)
        kv = dot(memory, w_kv, 1, 0).astype(BF16)
        kv_h = kv.reshape(-1, 2, kv_heads, head).transpose(1, 2, 0, 3)
        key_h, val_h = kv_h[0], kv_h[1]

        query = heads_of(dot(hid, w_q, 1, 0).astype(BF16))
        scale = head ** -0.5
        prob = jax.nn.softmax(bdot(query, key_h, 2, 2) * scale, axis=-1)
        prob_bf = prob.astype(BF16)
        ctx = flat_of(bdot(prob_bf, val_h, 2, 1).astype(BF16))
        mid = (hid.astype(F32) + dot(ctx, w_o, 1, 0)).astype(BF16)
        ctx_all = gather(ctx)
        dec_act, dec_gpre, g_mid = dec_mlp(mid, cot, w_1, w_2, w_1.shape[1] // 7)
        gpre_all = gather(dec_gpre)
        g_ctx = heads_of(dot(g_mid, w_o, 1, 1).astype(BF16))
        g_prob = bdot(g_ctx, val_h, 2, 2)
        g_val = bdot(prob_bf, g_ctx, 1, 1).astype(BF16)
        g_logit = (prob * (g_prob - jnp.sum(prob * g_prob, axis=-1, keepdims=True)) * scale).astype(BF16)
        g_key = bdot(g_logit, query, 1, 1).astype(BF16)
        g_kv = jnp.concatenate([g_key[i] for i in range(kv_heads)] + [g_val[i] for i in range(kv_heads)], axis=1)
        g_mem = dot(g_kv, w_kv, 1, 1).astype(BF16)

        kv_sib = swap(g_kv)
        gm_sib = dot(kv_sib, half(w_kv, 0, core), 1, 1).astype(BF16)
        own = lax.optimization_barrier(dot(act, half(g_mem, 1, core), 0, 0))
        down_half = own + dot(act_sib, gm_sib, 0, 0)
        down_half, g_mem, g_logit, g_mid, dec_gpre, kv_sib, mem_sib = lax.optimization_barrier((down_half, g_mem, g_logit, g_mid, dec_gpre, kv_sib, mem_sib))
        down_sum = scatter(down_half)

        def gpre_half(index):
            g_act = dot(g_mem, half(down, 0, index), 1, 1).astype(BF16)
            return jax.vjp(jax.nn.gelu, half(pre, 1, index))[1](g_act.astype(F32))[0].astype(BF16)

        gpre_send = gpre_half(1 - core)
        gpre_sib = swap(gpre_send)
        gpre_own = gpre_half(core)
        wkv_half = dot(memory, half(g_kv, 1, core), 0, 0) + dot(mem_sib, half(kv_sib, 1, core), 0, 0)
        own = lax.optimization_barrier(dot(x, gpre_own, 0, 0))
        up_half = with_layout_constraint(own + dot(x_sib, gpre_sib, 0, 0), Layout((0, 1)))
        up_half = with_layout_constraint(jnp.concatenate([up_half, wkv_half], axis=1), Layout((0, 1)))
        up_half, gpre_own, g_logit, g_mid, dec_gpre = lax.optimization_barrier((up_half, gpre_own, g_logit, g_mid, dec_gpre))
        up_sum = scatter(up_half)
        n1 = d_model // n_dev
        n2 = w_1.shape[1] // n_dev
        g_down = join(half(down_sum, 0, core), swap(half(down_sum, 0, 1 - core)))
        up_own, up_other = half(up_sum, 0, core), swap(half(up_sum, 0, 1 - core))
        n_ff = up_own.shape[1] - kv_width
        g_up = join(up_own[:, :n_ff], up_other[:, :n_ff])
        g_wkv = join(up_own[:, n_ff:], up_other[:, n_ff:])

        g_query = flat_of(bdot(g_logit, key_h, 2, 1).astype(BF16))
        dh = (g_mid.astype(F32) + dot(g_query, w_q, 1, 1)).astype(BF16)
        dh = lax.ppermute(dh, 'chip', partner_perm)

        sent = [t.reshape(s_dec, n_dev, -1) for t in (dec_act, g_mid, g_query, mid)]
        cols = lax.all_to_all(jnp.concatenate(sent, axis=2), AXES, split_axis=1, concat_axis=0, tiled=True)
        cols = cols.reshape(n_dev * s_dec, -1)
        gmid_c, mid_c = cols[:, n2:n2 + n1], cols[:, n2 + 2 * n1:]
        halves = cols.reshape(n_data, 2, chips // 2, 2 * s_dec, -1)
        cols = jnp.concatenate([halves[:, 1:], halves[:, :1]], axis=1).reshape(n_dev * s_dec, -1)
        act_c, gq_c = cols[:, :n2], cols[:, n2 + n1:n2 + 2 * n1]
        g_w2 = dot(act_c, cot_all, 0, 0)
        g_w1 = dot(mid_c, gpre_all, 0, 0)
        blocks = jnp.concatenate([dot(ctx_all, gmid_c, 0, 0), dot(hid_all, gq_c, 0, 0)], axis=1)
        blocks = lax.all_to_all(blocks.reshape(n_dev, n1, -1), AXES, split_axis=0, concat_axis=0, tiled=True)
        g_wo, g_wq = (b.transpose(1, 0, 2).reshape(n1, -1) for b in (blocks[:, :, :n1], blocks[:, :, n1:]))
        part = lax.optimization_barrier(dot(gpre_own, half(up, 1, core), 1, 1))
        dx = (g_mem.astype(F32) + part + dot(gpre_send, half(up, 1, 1 - core), 1, 1)).astype(BF16)
        g_wk = g_wkv[:, :kv_width].reshape(1, n1, kv_heads, head)
        g_wv = g_wkv[:, kv_width:].reshape(1, n1, kv_heads, head)
        return (dx[None], dh[None], g_up[None], g_down[None], g_wk, g_wv, g_wq[None], g_wo[None], g_w1[None], g_w2[None])

    return jax.shard_map(step, mesh=mesh,
                         in_specs=(row_spec, row_spec, row_spec, full_spec3, full_spec3, full_spec4, full_spec4, full_spec3, full_spec3, full_spec3, full_spec3),
                         out_specs=(row_spec, row_spec, grad_spec3, grad_spec3, grad_spec4, grad_spec4, grad_spec3, grad_spec3, grad_spec3, grad_spec3),
                         check_vma=False)
```
